256 devices in a mesh: phase: 2 (over core), space: 128 (over z, x, y).
Axes of the slice: x: 4, y: 4, z: 8, core: 2. Of those that a mesh axis runs over, the one named last changes fastest.
Arguments:
- features: bfloat16 [2, 65536, 256], P(None, 'space'), may hold values from -45 to 45
- weights: bfloat16 [2, 27, 256, 256], P('phase'), may hold values from -0.078125 to 0.078125
- conv_bias: float32 [2, 256], replicated, may hold values from -4 to 4
- rulebook: int32 [65536, 27], P('space'), may hold values from 0 to 1024, as said below
- border: int32 [128, 64], P('space'), may hold values from 0 to 511, as said below
- pull_slots: int32 [128, 128, 4], P('space'), may hold values from 0 to 63
Outputs:
- section_outputs: bfloat16 [2, 2, 65536, 256], P('phase', None, 'space')
The draws below stay inside these ranges and needn't reach their ends.
Inputs may be any that keep to these rules, and one draw needn't show every extreme that they name: `rulebook`: entries below 512 name a row of the voxel's own device, entries 512 + q * 4 + i name slot i pulled from device q, and the largest value means no neighbour; offset 27 // 2 always names the voxel itself. `border`: each device's entries are distinct rows of its own block.
All inputs are finite; a program needn't handle non-finite values.
Results may differ from the reference program's by a relative error of at most 0.0041.
Values may be sent and summed in bfloat16 or wider, within the bound.
A program may use at most 64 MiB of HBM per device.

```python
import jax
import jax.numpy as jnp
from jax import lax

C = 256
K = 27
MB = 2
CAP = 4
ROWS_DEV = 512
BORDER = 64
ROWS = 65536
N_SPACE = 128


def draw_features(key, part):
    key_base, key_rows, key_cols = jax.random.split(key, 3)
    base = jnp.clip(jax.random.normal(key_base, (MB, ROWS, C)), -5.0, 5.0)
    row_scale = jnp.exp(jax.random.uniform(key_rows, (MB, ROWS, 1), minval=jnp.log(0.3), maxval=jnp.log(3.0)))
    col_scale = jnp.exp(jax.random.uniform(key_cols, (1, 1, C), minval=jnp.log(0.3), maxval=jnp.log(3.0)))
    return (base * row_scale * col_scale).astype(jnp.bfloat16)


def draw_rulebook(key, part):
    key_kind, key_local, key_remote = jax.random.split(key, 3)
    kind = jax.random.randint(key_kind, (ROWS, K), 0, 10)
    local_code = jax.random.randint(key_local, (ROWS, K), 0, ROWS_DEV)
    remote_code = ROWS_DEV + jax.random.randint(key_remote, (ROWS, K), 0, N_SPACE * CAP)
    missing = jnp.full((ROWS, K), ROWS_DEV + N_SPACE * CAP, jnp.int32)
    code = jnp.where(kind < 5, local_code, jnp.where(kind < 8, remote_code, missing))
    own_row = (jnp.arange(ROWS, dtype=jnp.int32) % ROWS_DEV)[:, None]
    centre = (jnp.arange(K) == K // 2)[None, :]
    return jnp.where(centre, own_row, code).astype(jnp.int32)


def draw_border(key, part):
    device_keys = jax.random.split(key, N_SPACE)

    def one_device(device_key):
        return jax.random.permutation(device_key, ROWS_DEV)[:BORDER]
    return jax.vmap(one_device)(device_keys).astype(jnp.int32)


def place_ends(drawn, rng, low, largest):
    place = [jax.random.randint(jax.random.fold_in(rng, axis), (), 0, length) for axis, length in enumerate(drawn.shape)]
    widest = drawn.shape.index(max(drawn.shape))
    beside = place[:widest] + [(place[widest] + 1) % drawn.shape[widest]] + place[widest + 1:]
    return drawn.at[tuple(place)].set(low).at[tuple(beside)].set(largest)


def shard_levels(stream_key, extent, pieces, least, largest):
    def one(axis_at, shards_of):
        heights = jax.random.uniform(jax.random.fold_in(jax.random.fold_in(stream_key, 6), axis_at), (shards_of,), jnp.float32, least / len(pieces), largest / len(pieces))
        return jnp.repeat(jnp.exp(heights), extent[axis_at] // shards_of).reshape((-1,) + (1,) * (len(extent) - axis_at - 1))

    gain = one(*pieces[0])
    for cut in pieces[1:]:
        gain = gain * one(*cut)
    return gain


def centred(key, extent, scale, reach, pieces=(), kind=jnp.bfloat16):
    loudness = shard_levels(key, extent, pieces, -0.22, 0.18) if pieces else 1.0
    entries = jax.random.normal(key, extent, jnp.float32) * scale * loudness
    return jnp.minimum(jnp.maximum(entries, -reach), reach).astype(kind)


def setup_inputs(seed: int = 0) -> dict:
    streams_of = jax.random.split(jax.random.key(seed), 7)
    features = draw_features(jax.random.fold_in(streams_of[6], 71), 0)
    weights = centred(streams_of[1], (2, K, C, C), (K * C) ** -0.5, 0.078125, ((0, 2),))
    conv_bias = centred(streams_of[2], (2, C), 1.0, 4.0, (), jnp.float32)
    rulebook = draw_rulebook(jax.random.fold_in(streams_of[6], 71), 0)
    border = draw_border(jax.random.fold_in(streams_of[6], 71), 0)
    pull_slots = place_ends(jax.random.randint(streams_of[5], (N_SPACE, N_SPACE, CAP), 0, BORDER), jax.random.fold_in(streams_of[5], 1), 0, BORDER - 1).astype(jnp.int32)
    return dict(features=features, weights=weights, conv_bias=conv_bias, rulebook=rulebook, border=border, pull_slots=pull_slots)


def global_rows(rulebook, border, pull_slots):
    owner = (jnp.arange(ROWS, dtype=jnp.int32) // ROWS_DEV)[:, None]
    local_rows = owner * ROWS_DEV + rulebook
    remote_code = jnp.clip(rulebook - ROWS_DEV, 0, N_SPACE * CAP - 1).astype(jnp.int32)
    peer_index = remote_code // CAP
    slot_index = remote_code % CAP
    chosen = pull_slots[owner, peer_index, slot_index]
    remote_rows = peer_index * ROWS_DEV + border[peer_index, chosen]
    missing = jnp.full_like(rulebook, ROWS)
    return jnp.where(rulebook < ROWS_DEV, local_rows, jnp.where(rulebook < ROWS_DEV + N_SPACE * CAP, remote_rows, missing)).astype(jnp.int32)

def section(inputs, kernel, bias_row, neighbour):
    values = inputs.astype(jnp.float32)
    mean_square = lax.optimization_barrier(jnp.mean(values * values, axis=1, keepdims=True))
    normed = (values * lax.rsqrt(mean_square + 1e-06)).astype(jnp.bfloat16)
    extended = jnp.concatenate([normed, jnp.zeros((1, C), jnp.bfloat16)], axis=0)

    def add_offset(total, item):
        column, matrix = item
        return (total + jnp.dot(extended[column], matrix, preferred_element_type=jnp.float32), None)
    convolved, unused = lax.scan(add_offset, jnp.zeros((ROWS, C), jnp.float32), (neighbour.T, kernel))
    return (values + jax.nn.silu(convolved + bias_row)).astype(jnp.bfloat16)

def reference(features, weights, conv_bias, rulebook, border, pull_slots):
    neighbour = global_rows(rulebook, border, pull_slots)
    latents = []
    recons = []
    for batch_index in range(MB):
        latent = section(features[batch_index], weights[0], conv_bias[0], neighbour)
        latents.append(latent)
        recons.append(section(latent, weights[1], conv_bias[1], neighbour))
    return jnp.stack([jnp.stack(latents), jnp.stack(recons)])
```

```python
import functools

import jax
import jax.numpy as jnp
from jax import lax
from jax.experimental import pallas as pl
from jax.experimental.pallas import tpu as pltpu
from jax.sharding import PartitionSpec as P

BF16 = jnp.bfloat16
F32 = jnp.float32


def normalised(values):
    mean_square = jnp.mean(values * values, axis=1, keepdims=True)
    return (values * lax.rsqrt(mean_square + 1e-06)).astype(BF16)


def kernel(
    sizes, features, weights, bias, rulebook, border, wanted, out,
    kernels, onehot, chooser, normed, latent, total, slots, send, halo,
    slot_send, slot_recv, row_send, row_recv, swap_send, swap_recv, local_sems,
):
    peers, cap, rows, offsets, channels, extents = sizes
    phase = lax.axis_index("phase")
    me = lax.axis_index("space")
    halo_rows = peers * cap
    width = rows + halo_rows
    depth, breadth, height = extents

    def peer_at(step):
        swing = step // (breadth * height)
        far = depth // 2 + ((swing + 1) // 2) * (2 * (swing % 2) - 1)
        side = breadth // 2 + (step // height) % breadth
        up = height // 2 + step % height
        z = (me // (breadth * height) + far + depth) % depth
        x = ((me // height) % breadth + side) % breadth
        y = (me % height + up) % height
        return (z * breadth + x) * height + y

    def each_partner(action):
        @pl.loop(0, peers)
        def _(step):
            peer = peer_at(step)

            @pl.when(peer != me)
            def _():
                action(peer)

    barrier = pltpu.get_barrier_semaphore()
    each_partner(lambda peer: pl.semaphore_signal(barrier, inc=1, device_id={"space": peer}))
    pl.semaphore_signal(barrier, inc=1, device_id={"phase": 1 - phase})

    own_weights = pltpu.make_async_copy(weights.at[0], kernels.at[phase], local_sems.at[0])
    own_weights.start()
    pl.semaphore_wait(barrier, peers)

    own_slots = pltpu.make_async_copy(wanted.at[me], slots.at[me], local_sems.at[1])
    own_slots.start()

    def slot_copy(peer):
        return pltpu.make_async_remote_copy(
            src_ref=wanted.at[peer], dst_ref=slots.at[me], send_sem=slot_send, recv_sem=slot_recv,
            device_id={"space": peer},
        )
    each_partner(lambda peer: slot_copy(peer).start())

    swap = pltpu.make_async_remote_copy(
        src_ref=weights.at[0], dst_ref=kernels.at[phase], send_sem=swap_send.at[0], recv_sem=swap_recv.at[0],
        device_id={"phase": 1 - phase},
    )
    swap.start()

    block = 32
    codes_at = lax.broadcasted_iota(jnp.int32, (block, width), 1)

    @pl.loop(0, rows // block)
    def _(index):
        window = pl.ds(pl.multiple_of(index * block, block), block)
        codes = rulebook[window, :]
        for offset in range(offsets):
            hit = codes[:, offset:offset + 1] == codes_at
            onehot[offset, window, :] = jnp.where(hit, 1.0, 0.0).astype(BF16)

    normed[0] = normalised(features[phase].astype(F32))
    total[...] = jnp.zeros_like(total)

    def wait_all(buffer, send_sem, recv_sem):
        everything = buffer.at[pl.ds(0, peers - 1)]
        arrived = pltpu.make_async_remote_copy(
            src_ref=everything, dst_ref=everything, send_sem=send_sem, recv_sem=recv_sem,
            device_id={"space": me},
        )
        return arrived

    own_slots.wait()
    arrived = wait_all(slots, slot_send, slot_recv)
    arrived.wait_recv()

    borders = border.shape[1]
    square = (borders, borders)
    diagonal = lax.broadcasted_iota(jnp.int32, square, 0) == lax.broadcasted_iota(jnp.int32, square, 1)
    border_column = jnp.sum(jnp.where(diagonal, jnp.broadcast_to(border[...], square), 0), axis=1, keepdims=True)
    at_row = lax.broadcasted_iota(jnp.int32, (borders, rows), 1)
    border_hits = jnp.where(border_column == at_row, 1.0, 0.0).astype(BF16)
    repeat_row = lax.broadcasted_iota(jnp.int32, (halo_rows, peers), 0) // cap
    repeat = repeat_row == lax.broadcasted_iota(jnp.int32, (halo_rows, peers), 1)
    lanes = slots.shape[2]
    table = slots[:, 0, :].astype(F32).astype(BF16)
    spread = jnp.dot(jnp.where(repeat, 1.0, 0.0).astype(BF16), table, preferred_element_type=F32)
    slot_of = lax.broadcasted_iota(jnp.int32, (halo_rows, lanes), 0) % cap
    mine = slot_of == lax.broadcasted_iota(jnp.int32, (halo_rows, lanes), 1)
    slot_column = jnp.sum(jnp.where(mine, spread, 0.0), axis=1, keepdims=True)
    slot_hits = slot_column == lax.broadcasted_iota(jnp.int32, (halo_rows, borders), 1).astype(F32)
    chooser[...] = jnp.dot(
        jnp.where(slot_hits, 1.0, 0.0).astype(BF16), border_hits, preferred_element_type=F32
    ).astype(BF16)

    def gathered(section, first, table_rows):
        @pl.loop(0, offsets)
        def _(offset):
            picked = jnp.dot(
                onehot[offset, :, first:first + table_rows.shape[0]], table_rows, preferred_element_type=F32
            ).astype(BF16)
            total[...] += jnp.dot(picked, kernels[section, offset], preferred_element_type=F32)

    for section in range(2):
        chosen = jnp.dot(chooser[...], normed[section], preferred_element_type=F32)
        send[section] = chosen.reshape(peers, cap, channels).astype(BF16)
        own_rows = pltpu.make_async_copy(send.at[section, me], halo.at[section, me], local_sems.at[2 + section])
        own_rows.start()

        def row_copy(peer):
            return pltpu.make_async_remote_copy(
                src_ref=send.at[section, peer], dst_ref=halo.at[section, me],
                send_sem=row_send.at[section], recv_sem=row_recv.at[section], device_id={"space": peer},
            )
        each_partner(lambda peer: row_copy(peer).start())
        if section == 0:
            own_weights.wait()
            swap.wait()
        gathered(section, 0, normed[section])
        own_rows.wait()
        wait_all(halo.at[section], row_send.at[section], row_recv.at[section]).wait_recv()
        arrived_rows = halo[section].astype(F32).reshape(halo_rows, channels).astype(BF16)
        gathered(section, rows, arrived_rows)
        summed = total[...] + bias[section:section + 1, :]
        source = features[phase] if section == 0 else latent[0]
        values = source.astype(F32) + summed / (1.0 + jnp.exp(-summed))
        latent[section] = values.astype(BF16)
        if section == 0:
            normed[1] = normalised(latent[0].astype(F32))
            total[...] = jnp.zeros_like(total)

        def result_copy():
            return pltpu.make_async_remote_copy(
                src_ref=latent.at[section], dst_ref=out.at[0, phase],
                send_sem=swap_send.at[1], recv_sem=swap_recv.at[1], device_id={"phase": 1 - phase},
            )
        kept = pltpu.make_async_copy(latent.at[section], out.at[0, phase], local_sems.at[4])

        @pl.when(phase == section)
        def _():
            kept.start()

        @pl.when(phase != section)
        def _():
            result_copy().start()

    @pl.when(phase == 0)
    def _():
        pltpu.make_async_copy(latent.at[0], out.at[0, 0], local_sems.at[4]).wait()

    @pl.when(phase == 1)
    def _():
        pltpu.make_async_copy(latent.at[1], out.at[0, 1], local_sems.at[4]).wait()
    pair = pltpu.make_async_remote_copy(
        src_ref=latent.at[0], dst_ref=out.at[0, 1 - phase],
        send_sem=swap_send.at[1], recv_sem=swap_recv.at[1], device_id={"phase": 1 - phase},
    )
    pair.wait()
    arrived.wait_send()
    for section in range(2):
        wait_all(send.at[section], row_send.at[section], row_recv.at[section]).wait_send()


def body(extents, features, weights, conv_bias, rulebook, border, pull_slots):
    micro, rows, channels = features.shape
    offsets = rulebook.shape[1]
    peers, cap = pull_slots.shape[1:]
    lanes = 128
    wanted = jnp.pad(pull_slots[0], ((0, 0), (0, lanes - cap)))[:, None, :]
    sizes = (peers, cap, rows, offsets, channels, extents)
    width = rows + peers * cap
    vmem = pl.BlockSpec(memory_space=pltpu.VMEM)
    anywhere = pl.BlockSpec(memory_space=pl.ANY)
    return pl.pallas_call(
        functools.partial(kernel, sizes),
        out_shape=jax.ShapeDtypeStruct((1, micro, rows, channels), BF16),
        in_specs=[vmem, anywhere, vmem, vmem, vmem, vmem],
        out_specs=anywhere,
        scratch_shapes=[
            pltpu.VMEM((2, offsets, channels, channels), BF16),
            pltpu.VMEM((offsets, rows, width), BF16),
            pltpu.VMEM((peers * cap, rows), BF16),
            pltpu.VMEM((2, rows, channels), BF16),
            pltpu.VMEM((2, rows, channels), BF16),
            pltpu.VMEM((rows, channels), F32),
            pltpu.VMEM((peers, 1, lanes), jnp.int32),
            pltpu.VMEM((2, peers, cap, channels), BF16),
            pltpu.VMEM((2, peers, cap, channels), BF16),
            pltpu.SemaphoreType.DMA,
            pltpu.SemaphoreType.DMA,
            pltpu.SemaphoreType.DMA((2,)),
            pltpu.SemaphoreType.DMA((2,)),
            pltpu.SemaphoreType.DMA((2,)),
            pltpu.SemaphoreType.DMA((2,)),
            pltpu.SemaphoreType.DMA((5,)),
        ],
        compiler_params=pltpu.CompilerParams(
            collective_id=0, has_side_effects=True, vmem_limit_bytes=60 * 1024 * 1024
        ),
        name="autoencoder",
    )(features, weights, conv_bias, rulebook, border, wanted)


def solution(mesh):
    space = mesh.shape["space"]
    extents = (space // 16, 4, 4) if space % 16 == 0 else (space, 1, 1)
    return jax.shard_map(
        functools.partial(body, extents),
        mesh=mesh,
        in_specs=(
            P(None, "space", None),
            P("phase", None, None, None),
            P(),
            P("space", None),
            P("space", None),
            P("space", None, None),
        ),
        out_specs=P("phase", None, "space", None),
        check_vma=False,
    )
```

```python
import functools

import jax
import jax.numpy as jnp
from jax import lax
from jax.experimental import pallas as pl
from jax.experimental.pallas import tpu as pltpu
from jax.sharding import PartitionSpec as P

BF16 = jnp.bfloat16
F32 = jnp.float32


def normalised(values):
    mean_square = jnp.mean(values * values, axis=1, keepdims=True)
    return (values * lax.rsqrt(mean_square + 1e-06)).astype(BF16)


def kernel(
    sizes, features, weights, bias, rulebook, border, wanted, out,
    kernels, onehot, chooser, normed, latent, total, slots, send, halo,
    slot_send, slot_recv, row_send, row_recv, swap_send, swap_recv, local_sems,
):
    peers, cap, rows, offsets, channels, extents = sizes
    phase = lax.axis_index("phase")
    me = lax.axis_index("space")
    halo_rows = peers * cap
    width = rows + halo_rows
    depth, breadth, height = extents

    def peer_at(step):
        swing = step // (breadth * height)
        far = depth // 2 + ((swing + 1) // 2) * (2 * (swing % 2) - 1)
        side = breadth // 2 + (step // height) % breadth
        up = height // 2 + step % height
        z = (me // (breadth * height) + far + depth) % depth
        x = ((me // height) % breadth + side) % breadth
        y = (me % height + up) % height
        return (z * breadth + x) * height + y

    def each_partner(action):
        @pl.loop(0, peers)
        def _(step):
            peer = peer_at(step)

            @pl.when(peer != me)
            def _():
                action(peer)

    barrier = pltpu.get_barrier_semaphore()
    each_partner(lambda peer: pl.semaphore_signal(barrier, inc=1, device_id={"space": peer}))
    pl.semaphore_signal(barrier, inc=1, device_id={"phase": 1 - phase})

    own_weights = pltpu.make_async_copy(weights.at[0], kernels.at[phase], local_sems.at[0])
    own_weights.start()
    pl.semaphore_wait(barrier, peers)

    own_slots = pltpu.make_async_copy(wanted.at[me], slots.at[me], local_sems.at[1])
    own_slots.start()

    def slot_copy(peer):
        return pltpu.make_async_remote_copy(
            src_ref=wanted.at[peer], dst_ref=slots.at[me], send_sem=slot_send, recv_sem=slot_recv,
            device_id={"space": peer},
        )
    each_partner(lambda peer: slot_copy(peer).start())

    swap = pltpu.make_async_remote_copy(
        src_ref=weights.at[0], dst_ref=kernels.at[phase], send_sem=swap_send.at[0], recv_sem=swap_recv.at[0],
        device_id={"phase": 1 - phase},
    )
    swap.start()

    block = 32
    codes_at = lax.broadcasted_iota(jnp.int32, (block, width), 1)

    @pl.loop(0, rows // block)
    def _(index):
        window = pl.ds(pl.multiple_of(index * block, block), block)
        codes = rulebook[window, :]
        for offset in range(offsets):
            hit = codes[:, offset:offset + 1] == codes_at
            onehot[offset, window, :] = jnp.where(hit, 1.0, 0.0).astype(BF16)

    normed[0] = normalised(features[phase].astype(F32))
    total[...] = jnp.zeros_like(total)

    def wait_all(buffer, send_sem, recv_sem):
        everything = buffer.at[pl.ds(0, peers - 1)]
        arrived = pltpu.make_async_remote_copy(
            src_ref=everything, dst_ref=everything, send_sem=send_sem, recv_sem=recv_sem,
            device_id={"space": me},
        )
        return arrived

    own_slots.wait()
    arrived = wait_all(slots, slot_send, slot_recv)
    arrived.wait_recv()

    borders = border.shape[1]
    square = (borders, borders)
    diagonal = lax.broadcasted_iota(jnp.int32, square, 0) == lax.broadcasted_iota(jnp.int32, square, 1)
    border_column = jnp.sum(jnp.where(diagonal, jnp.broadcast_to(border[...], square), 0), axis=1, keepdims=True)
    at_row = lax.broadcasted_iota(jnp.int32, (borders, rows), 1)
    border_hits = jnp.where(border_column == at_row, 1.0, 0.0).astype(BF16)
    repeat_row = lax.broadcasted_iota(jnp.int32, (halo_rows, peers), 0) // cap
    repeat = repeat_row == lax.broadcasted_iota(jnp.int32, (halo_rows, peers), 1)
    lanes = slots.shape[2]
    table = slots[:, 0, :].astype(F32).astype(BF16)
    spread = jnp.dot(jnp.where(repeat, 1.0, 0.0).astype(BF16), table, preferred_element_type=F32)
    slot_of = lax.broadcasted_iota(jnp.int32, (halo_rows, lanes), 0) % cap
    mine = slot_of == lax.broadcasted_iota(jnp.int32, (halo_rows, lanes), 1)
    slot_column = jnp.sum(jnp.where(mine, spread, 0.0), axis=1, keepdims=True)
    slot_hits = slot_column == lax.broadcasted_iota(jnp.int32, (halo_rows, borders), 1).astype(F32)
    chooser[...] = jnp.dot(
        jnp.where(slot_hits, 1.0, 0.0).astype(BF16), border_hits, preferred_element_type=F32
    ).astype(BF16)

    part = 256

    def gathered(section, first, table_rows):
        @pl.loop(0, rows // part)
        def _(index):
            window = pl.ds(pl.multiple_of(index * part, part), part)
            summed = total[window, :]
            for offset in range(offsets):
                picked = jnp.dot(
                    onehot[offset, window, first:first + table_rows.shape[0]], table_rows, preferred_element_type=F32
                ).astype(BF16)
                summed = summed + jnp.dot(picked, kernels[section, offset], preferred_element_type=F32)
            total[window, :] = summed

    for section in range(2):
        chosen = jnp.dot(chooser[...], normed[section], preferred_element_type=F32)
        send[section] = chosen.reshape(peers, cap, channels).astype(BF16)
        own_rows = pltpu.make_async_copy(send.at[section, me], halo.at[section, me], local_sems.at[2 + section])
        own_rows.start()

        def row_copy(peer):
            return pltpu.make_async_remote_copy(
                src_ref=send.at[section, peer], dst_ref=halo.at[section, me],
                send_sem=row_send.at[section], recv_sem=row_recv.at[section], device_id={"space": peer},
            )
        each_partner(lambda peer: row_copy(peer).start())
        if section == 0:
            own_weights.wait()
            swap.wait()
        gathered(section, 0, normed[section])
        own_rows.wait()
        wait_all(halo.at[section], row_send.at[section], row_recv.at[section]).wait_recv()
        arrived_rows = halo[section].astype(F32).reshape(halo_rows, channels).astype(BF16)
        gathered(section, rows, arrived_rows)
        summed = total[...] + bias[section:section + 1, :]
        source = features[phase] if section == 0 else latent[0]
        values = source.astype(F32) + summed / (1.0 + jnp.exp(-summed))
        latent[section] = values.astype(BF16)
        if section == 0:
            normed[1] = normalised(latent[0].astype(F32))
            total[...] = jnp.zeros_like(total)

        def result_copy():
            return pltpu.make_async_remote_copy(
                src_ref=latent.at[section], dst_ref=out.at[0, phase],
                send_sem=swap_send.at[1], recv_sem=swap_recv.at[1], device_id={"phase": 1 - phase},
            )
        kept = pltpu.make_async_copy(latent.at[section], out.at[0, phase], local_sems.at[4])

        @pl.when(phase == section)
        def _():
            kept.start()

        @pl.when(phase != section)
        def _():
            result_copy().start()

    @pl.when(phase == 0)
    def _():
        pltpu.make_async_copy(latent.at[0], out.at[0, 0], local_sems.at[4]).wait()

    @pl.when(phase == 1)
    def _():
        pltpu.make_async_copy(latent.at[1], out.at[0, 1], local_sems.at[4]).wait()
    pair = pltpu.make_async_remote_copy(
        src_ref=latent.at[0], dst_ref=out.at[0, 1 - phase],
        send_sem=swap_send.at[1], recv_sem=swap_recv.at[1], device_id={"phase": 1 - phase},
    )
    pair.wait()
    arrived.wait_send()
    for section in range(2):
        wait_all(send.at[section], row_send.at[section], row_recv.at[section]).wait_send()


def body(extents, features, weights, conv_bias, rulebook, border, pull_slots):
    micro, rows, channels = features.shape
    offsets = rulebook.shape[1]
    peers, cap = pull_slots.shape[1:]
    lanes = 128
    wanted = jnp.pad(pull_slots[0], ((0, 0), (0, lanes - cap)))[:, None, :]
    sizes = (peers, cap, rows, offsets, channels, extents)
    width = rows + peers * cap
    vmem = pl.BlockSpec(memory_space=pltpu.VMEM)
    anywhere = pl.BlockSpec(memory_space=pl.ANY)
    return pl.pallas_call(
        functools.partial(kernel, sizes),
        out_shape=jax.ShapeDtypeStruct((1, micro, rows, channels), BF16),
        in_specs=[vmem, anywhere, vmem, vmem, vmem, vmem],
        out_specs=anywhere,
        scratch_shapes=[
            pltpu.VMEM((2, offsets, channels, channels), BF16),
            pltpu.VMEM((offsets, rows, width), BF16),
            pltpu.VMEM((peers * cap, rows), BF16),
            pltpu.VMEM((2, rows, channels), BF16),
            pltpu.VMEM((2, rows, channels), BF16),
            pltpu.VMEM((rows, channels), F32),
            pltpu.VMEM((peers, 1, lanes), jnp.int32),
            pltpu.VMEM((2, peers, cap, channels), BF16),
            pltpu.VMEM((2, peers, cap, channels), BF16),
            pltpu.SemaphoreType.DMA,
            pltpu.SemaphoreType.DMA,
            pltpu.SemaphoreType.DMA((2,)),
            pltpu.SemaphoreType.DMA((2,)),
            pltpu.SemaphoreType.DMA((2,)),
            pltpu.SemaphoreType.DMA((2,)),
            pltpu.SemaphoreType.DMA((5,)),
        ],
        compiler_params=pltpu.CompilerParams(
            collective_id=0, has_side_effects=True, vmem_limit_bytes=60 * 1024 * 1024
        ),
        name="autoencoder",
    )(features, weights, conv_bias, rulebook, border, wanted)


def solution(mesh):
    space = mesh.shape["space"]
    extents = (space // 16, 4, 4) if space % 16 == 0 else (space, 1, 1)
    return jax.shard_map(
        functools.partial(body, extents),
        mesh=mesh,
        in_specs=(
            P(None, "space", None),
            P("phase", None, None, None),
            P(),
            P("space", None),
            P("space", None),
            P("space", None, None),
        ),
        out_specs=P("phase", None, "space", None),
        check_vma=False,
    )
```

```python
import functools

import jax
import jax.numpy as jnp
from jax import lax
from jax.experimental import pallas as pl
from jax.experimental.pallas import tpu as pltpu
from jax.sharding import PartitionSpec as P

BF16 = jnp.bfloat16
F32 = jnp.float32


def normalised(values):
    mean_square = jnp.mean(values * values, axis=1, keepdims=True)
    return (values * lax.rsqrt(mean_square + 1e-06)).astype(BF16)


def kernel(
    sizes, features, weights, bias, rulebook, border, wanted, out,
    kernels, onehot, chooser, normed, latent, total, slots, send, halo,
    slot_send, slot_recv, row_send, row_recv, swap_send, swap_recv, local_sems,
):
    peers, cap, rows, offsets, channels = sizes
    phase = lax.axis_index("phase")
    me = lax.axis_index("space")
    halo_rows = peers * cap
    width = rows + halo_rows

    def each_partner(action):
        middle, odd = peers // 2, peers % 2

        def act(shift):
            action(lax.rem(me + shift, peers))
        if not odd:
            act(middle)

        @pl.loop(1, middle + odd)
        def _(step):
            act(middle + odd - step)
            act(middle + step)

    barrier = pltpu.get_barrier_semaphore()
    each_partner(lambda peer: pl.semaphore_signal(barrier, inc=1, device_id={"space": peer}))
    pl.semaphore_signal(barrier, inc=1, device_id={"phase": 1 - phase})

    own_weights = pltpu.make_async_copy(weights.at[0], kernels.at[phase], local_sems.at[0])
    own_weights.start()
    pl.semaphore_wait(barrier, peers)

    own_slots = pltpu.make_async_copy(wanted.at[me], slots.at[me], local_sems.at[1])
    own_slots.start()

    def slot_copy(peer):
        return pltpu.make_async_remote_copy(
            src_ref=wanted.at[peer], dst_ref=slots.at[me], send_sem=slot_send, recv_sem=slot_recv,
            device_id={"space": peer},
        )
    each_partner(lambda peer: slot_copy(peer).start())

    swap = pltpu.make_async_remote_copy(
        src_ref=weights.at[0], dst_ref=kernels.at[phase], send_sem=swap_send.at[0], recv_sem=swap_recv.at[0],
        device_id={"phase": 1 - phase},
    )
    swap.start()

    block = 32
    codes_at = lax.broadcasted_iota(jnp.int32, (block, width), 1)

    @pl.loop(0, rows // block)
    def _(index):
        window = pl.ds(pl.multiple_of(index * block, block), block)
        codes = rulebook[window, :]
        for offset in range(offsets):
            hit = codes[:, offset:offset + 1] == codes_at
            onehot[offset, window, :] = jnp.where(hit, 1.0, 0.0).astype(BF16)

    normed[0] = normalised(features[phase].astype(F32))
    total[...] = jnp.zeros_like(total)

    def wait_all(buffer, send_sem, recv_sem):
        everything = buffer.at[pl.ds(0, peers - 1)]
        arrived = pltpu.make_async_remote_copy(
            src_ref=everything, dst_ref=everything, send_sem=send_sem, recv_sem=recv_sem,
            device_id={"space": me},
        )
        return arrived

    own_slots.wait()
    arrived = wait_all(slots, slot_send, slot_recv)
    arrived.wait_recv()

    borders = border.shape[1]
    square = (borders, borders)
    diagonal = lax.broadcasted_iota(jnp.int32, square, 0) == lax.broadcasted_iota(jnp.int32, square, 1)
    border_column = jnp.sum(jnp.where(diagonal, jnp.broadcast_to(border[...], square), 0), axis=1, keepdims=True)
    at_row = lax.broadcasted_iota(jnp.int32, (borders, rows), 1)
    border_hits = jnp.where(border_column == at_row, 1.0, 0.0).astype(BF16)
    repeat_row = lax.broadcasted_iota(jnp.int32, (halo_rows, peers), 0) // cap
    repeat = repeat_row == lax.broadcasted_iota(jnp.int32, (halo_rows, peers), 1)
    lanes = slots.shape[2]
    table = slots[:, 0, :].astype(F32).astype(BF16)
    spread = jnp.dot(jnp.where(repeat, 1.0, 0.0).astype(BF16), table, preferred_element_type=F32)
    slot_of = lax.broadcasted_iota(jnp.int32, (halo_rows, lanes), 0) % cap
    mine = slot_of == lax.broadcasted_iota(jnp.int32, (halo_rows, lanes), 1)
    slot_column = jnp.sum(jnp.where(mine, spread, 0.0), axis=1, keepdims=True)
    slot_hits = slot_column == lax.broadcasted_iota(jnp.int32, (halo_rows, borders), 1).astype(F32)
    chooser[...] = jnp.dot(
        jnp.where(slot_hits, 1.0, 0.0).astype(BF16), border_hits, preferred_element_type=F32
    ).astype(BF16)

    part = 256

    def gathered(section, first, table_rows):
        @pl.loop(0, rows // part)
        def _(index):
            window = pl.ds(pl.multiple_of(index * part, part), part)
            summed = total[window, :]
            for offset in range(offsets):
                picked = jnp.dot(
                    onehot[offset, window, first:first + table_rows.shape[0]], table_rows, preferred_element_type=F32
                ).astype(BF16)
                summed = summed + jnp.dot(picked, kernels[section, offset], preferred_element_type=F32)
            total[window, :] = summed

    for section in range(2):
        chosen = jnp.dot(chooser[...], normed[section], preferred_element_type=F32)
        send[section] = chosen.reshape(peers, cap, channels).astype(BF16)
        own_rows = pltpu.make_async_copy(send.at[section, me], halo.at[section, me], local_sems.at[2 + section])
        own_rows.start()

        def row_copy(peer):
            return pltpu.make_async_remote_copy(
                src_ref=send.at[section, peer], dst_ref=halo.at[section, me],
                send_sem=row_send.at[section], recv_sem=row_recv.at[section], device_id={"space": peer},
            )
        each_partner(lambda peer: row_copy(peer).start())
        if section == 0:
            own_weights.wait()
            swap.wait()
        gathered(section, 0, normed[section])
        own_rows.wait()
        wait_all(halo.at[section], row_send.at[section], row_recv.at[section]).wait_recv()
        arrived_rows = halo[section].astype(F32).reshape(halo_rows, channels).astype(BF16)
        gathered(section, rows, arrived_rows)
        summed = total[...] + bias[section:section + 1, :]
        source = features[phase] if section == 0 else latent[0]
        values = source.astype(F32) + summed / (1.0 + jnp.exp(-summed))
        latent[section] = values.astype(BF16)
        if section == 0:
            normed[1] = normalised(latent[0].astype(F32))
            total[...] = jnp.zeros_like(total)

        def result_copy():
            return pltpu.make_async_remote_copy(
                src_ref=latent.at[section], dst_ref=out.at[0, phase],
                send_sem=swap_send.at[1], recv_sem=swap_recv.at[1], device_id={"phase": 1 - phase},
            )
        kept = pltpu.make_async_copy(latent.at[section], out.at[0, phase], local_sems.at[4])

        @pl.when(phase == section)
        def _():
            kept.start()

        @pl.when(phase != section)
        def _():
            result_copy().start()

    @pl.when(phase == 0)
    def _():
        pltpu.make_async_copy(latent.at[0], out.at[0, 0], local_sems.at[4]).wait()

    @pl.when(phase == 1)
    def _():
        pltpu.make_async_copy(latent.at[1], out.at[0, 1], local_sems.at[4]).wait()
    pair = pltpu.make_async_remote_copy(
        src_ref=latent.at[0], dst_ref=out.at[0, 1 - phase],
        send_sem=swap_send.at[1], recv_sem=swap_recv.at[1], device_id={"phase": 1 - phase},
    )
    pair.wait()
    arrived.wait_send()
    for section in range(2):
        wait_all(send.at[section], row_send.at[section], row_recv.at[section]).wait_send()


def body(features, weights, conv_bias, rulebook, border, pull_slots):
    micro, rows, channels = features.shape
    offsets = rulebook.shape[1]
    peers, cap = pull_slots.shape[1:]
    lanes = 128
    wanted = jnp.pad(pull_slots[0], ((0, 0), (0, lanes - cap)))[:, None, :]
    sizes = (peers, cap, rows, offsets, channels)
    width = rows + peers * cap
    vmem = pl.BlockSpec(memory_space=pltpu.VMEM)
    anywhere = pl.BlockSpec(memory_space=pl.ANY)
    return pl.pallas_call(
        functools.partial(kernel, sizes),
        out_shape=jax.ShapeDtypeStruct((1, micro, rows, channels), BF16),
        in_specs=[vmem, anywhere, vmem, vmem, vmem, vmem],
        out_specs=anywhere,
        scratch_shapes=[
            pltpu.VMEM((2, offsets, channels, channels), BF16),
            pltpu.VMEM((offsets, rows, width), BF16),
            pltpu.VMEM((peers * cap, rows), BF16),
            pltpu.VMEM((2, rows, channels), BF16),
            pltpu.VMEM((2, rows, channels), BF16),
            pltpu.VMEM((rows, channels), F32),
            pltpu.VMEM((peers, 1, lanes), jnp.int32),
            pltpu.VMEM((2, peers, cap, channels), BF16),
            pltpu.VMEM((2, peers, cap, channels), BF16),
            pltpu.SemaphoreType.DMA,
            pltpu.SemaphoreType.DMA,
            pltpu.SemaphoreType.DMA((2,)),
            pltpu.SemaphoreType.DMA((2,)),
            pltpu.SemaphoreType.DMA((2,)),
            pltpu.SemaphoreType.DMA((2,)),
            pltpu.SemaphoreType.DMA((5,)),
        ],
        compiler_params=pltpu.CompilerParams(
            collective_id=0, has_side_effects=True, vmem_limit_bytes=60 * 1024 * 1024
        ),
        name="autoencoder",
    )(features, weights, conv_bias, rulebook, border, wanted)


def solution(mesh):
    return jax.shard_map(
        body,
        mesh=mesh,
        in_specs=(
            P(None, "space", None),
            P("phase", None, None, None),
            P(),
            P("space", None),
            P("space", None),
            P("space", None, None),
        ),
        out_specs=P("phase", None, "space", None),
        check_vma=False,
    )
```

```python
import functools

import jax
import jax.numpy as jnp
from jax import lax
from jax.experimental import pallas as pl
from jax.experimental.pallas import tpu as pltpu
from jax.sharding import PartitionSpec as P

BF16 = jnp.bfloat16
F32 = jnp.float32


def normalised(values):
    mean_square = jnp.mean(values * values, axis=1, keepdims=True)
    return (values * lax.rsqrt(mean_square + 1e-06)).astype(BF16)


def kernel(
    sizes, features, weights, bias, rulebook, border, wanted, out,
    kernels, onehot, chooser, normed, latent, total, slots, send, halo,
    slot_send, slot_recv, row_send, row_recv, swap_send, swap_recv, local_sems,
):
    peers, cap, rows, offsets, channels = sizes
    phase = lax.axis_index("phase")
    me = lax.axis_index("space")
    halo_rows = peers * cap
    width = rows + halo_rows

    def each_partner(action):
        middle, odd = peers // 2, peers % 2

        def act(shift):
            action(lax.rem(me + shift, peers))
        if not odd:
            act(middle)

        @pl.loop(1, middle + odd)
        def _(step):
            act(middle + odd - step)
            act(middle + step)

    barrier = pltpu.get_barrier_semaphore()
    each_partner(lambda peer: pl.semaphore_signal(barrier, inc=1, device_id={"space": peer}))
    pl.semaphore_signal(barrier, inc=1, device_id={"phase": 1 - phase})

    own_weights = pltpu.make_async_copy(weights.at[0], kernels.at[phase], local_sems.at[0])
    own_weights.start()
    pl.semaphore_wait(barrier, peers)

    own_slots = pltpu.make_async_copy(wanted.at[me], slots.at[me], local_sems.at[1])
    own_slots.start()

    def slot_copy(peer):
        return pltpu.make_async_remote_copy(
            src_ref=wanted.at[peer], dst_ref=slots.at[me], send_sem=slot_send, recv_sem=slot_recv,
            device_id={"space": peer},
        )
    each_partner(lambda peer: slot_copy(peer).start())

    swap = pltpu.make_async_remote_copy(
        src_ref=weights.at[0], dst_ref=kernels.at[phase], send_sem=swap_send.at[0], recv_sem=swap_recv.at[0],
        device_id={"phase": 1 - phase},
    )
    swap.start()

    block = 32
    codes_at = lax.broadcasted_iota(jnp.int16, (block, width), 1)
    ones, zeros = jnp.ones((block, width), BF16), jnp.zeros((block, width), BF16)

    @pl.loop(0, rows // block)
    def _(index):
        window = pl.ds(pl.multiple_of(index * block, block), block)
        codes = rulebook[window, :]
        for offset in range(offsets):
            code = jnp.broadcast_to(codes[:, offset:offset + 1], (block, width)).astype(jnp.int16)
            onehot[offset, window, :] = jnp.where(code == codes_at, ones, zeros)

    normed[0] = normalised(features[phase].astype(F32))
    total[...] = jnp.zeros_like(total)

    def wait_all(buffer, send_sem, recv_sem):
        everything = buffer.at[pl.ds(0, peers - 1)]
        arrived = pltpu.make_async_remote_copy(
            src_ref=everything, dst_ref=everything, send_sem=send_sem, recv_sem=recv_sem,
            device_id={"space": me},
        )
        return arrived

    own_slots.wait()
    arrived = wait_all(slots, slot_send, slot_recv)
    arrived.wait_recv()

    borders = border.shape[1]
    square = (borders, borders)
    diagonal = lax.broadcasted_iota(jnp.int32, square, 0) == lax.broadcasted_iota(jnp.int32, square, 1)
    border_column = jnp.sum(jnp.where(diagonal, jnp.broadcast_to(border[...], square), 0), axis=1, keepdims=True)
    at_row = lax.broadcasted_iota(jnp.int32, (borders, rows), 1)
    border_hits = jnp.where(border_column == at_row, 1.0, 0.0).astype(BF16)
    repeat_row = lax.broadcasted_iota(jnp.int32, (halo_rows, peers), 0) // cap
    repeat = repeat_row == lax.broadcasted_iota(jnp.int32, (halo_rows, peers), 1)
    lanes = slots.shape[2]
    table = slots[:, 0, :].astype(F32).astype(BF16)
    spread = jnp.dot(jnp.where(repeat, 1.0, 0.0).astype(BF16), table, preferred_element_type=F32)
    slot_of = lax.broadcasted_iota(jnp.int32, (halo_rows, lanes), 0) % cap
    mine = slot_of == lax.broadcasted_iota(jnp.int32, (halo_rows, lanes), 1)
    slot_column = jnp.sum(jnp.where(mine, spread, 0.0), axis=1, keepdims=True)
    slot_hits = slot_column == lax.broadcasted_iota(jnp.int32, (halo_rows, borders), 1).astype(F32)
    chooser[...] = jnp.dot(
        jnp.where(slot_hits, 1.0, 0.0).astype(BF16), border_hits, preferred_element_type=F32
    ).astype(BF16)

    part = 256

    def gathered(section, first, table_rows):
        @pl.loop(0, rows // part)
        def _(index):
            window = pl.ds(pl.multiple_of(index * part, part), part)
            summed = total[window, :]
            for offset in range(offsets):
                picked = jnp.dot(
                    onehot[offset, window, first:first + table_rows.shape[0]], table_rows, preferred_element_type=F32
                ).astype(BF16)
                summed = summed + jnp.dot(picked, kernels[section, offset], preferred_element_type=F32)
            total[window, :] = summed

    for section in range(2):
        chosen = jnp.dot(chooser[...], normed[section], preferred_element_type=F32)
        send[section] = chosen.reshape(peers, cap, channels).astype(BF16)
        own_rows = pltpu.make_async_copy(send.at[section, me], halo.at[section, me], local_sems.at[2 + section])
        own_rows.start()

        def row_copy(peer):
            return pltpu.make_async_remote_copy(
                src_ref=send.at[section, peer], dst_ref=halo.at[section, me],
                send_sem=row_send.at[section], recv_sem=row_recv.at[section], device_id={"space": peer},
            )
        each_partner(lambda peer: row_copy(peer).start())
        if section == 0:
            own_weights.wait()
            swap.wait()
        gathered(section, 0, normed[section])
        own_rows.wait()
        wait_all(halo.at[section], row_send.at[section], row_recv.at[section]).wait_recv()
        arrived_rows = halo[section].astype(F32).reshape(halo_rows, channels).astype(BF16)
        gathered(section, rows, arrived_rows)
        summed = total[...] + bias[section:section + 1, :]
        source = features[phase] if section == 0 else latent[0]
        values = source.astype(F32) + summed / (1.0 + jnp.exp(-summed))
        latent[section] = values.astype(BF16)
        if section == 0:
            normed[1] = normalised(latent[0].astype(F32))
            total[...] = jnp.zeros_like(total)

        def result_copy():
            return pltpu.make_async_remote_copy(
                src_ref=latent.at[section], dst_ref=out.at[0, phase],
                send_sem=swap_send.at[1], recv_sem=swap_recv.at[1], device_id={"phase": 1 - phase},
            )
        kept = pltpu.make_async_copy(latent.at[section], out.at[0, phase], local_sems.at[4])

        @pl.when(phase == section)
        def _():
            kept.start()

        @pl.when(phase != section)
        def _():
            result_copy().start()

    @pl.when(phase == 0)
    def _():
        pltpu.make_async_copy(latent.at[0], out.at[0, 0], local_sems.at[4]).wait()

    @pl.when(phase == 1)
    def _():
        pltpu.make_async_copy(latent.at[1], out.at[0, 1], local_sems.at[4]).wait()
    pair = pltpu.make_async_remote_copy(
        src_ref=latent.at[0], dst_ref=out.at[0, 1 - phase],
        send_sem=swap_send.at[1], recv_sem=swap_recv.at[1], device_id={"phase": 1 - phase},
    )
    pair.wait()
    arrived.wait_send()
    for section in range(2):
        wait_all(send.at[section], row_send.at[section], row_recv.at[section]).wait_send()


def body(features, weights, conv_bias, rulebook, border, pull_slots):
    micro, rows, channels = features.shape
    offsets = rulebook.shape[1]
    peers, cap = pull_slots.shape[1:]
    lanes = 128
    wanted = jnp.pad(pull_slots[0], ((0, 0), (0, lanes - cap)))[:, None, :]
    sizes = (peers, cap, rows, offsets, channels)
    width = rows + peers * cap
    vmem = pl.BlockSpec(memory_space=pltpu.VMEM)
    anywhere = pl.BlockSpec(memory_space=pl.ANY)
    return pl.pallas_call(
        functools.partial(kernel, sizes),
        out_shape=jax.ShapeDtypeStruct((1, micro, rows, channels), BF16),
        in_specs=[vmem, anywhere, vmem, vmem, vmem, vmem],
        out_specs=anywhere,
        scratch_shapes=[
            pltpu.VMEM((2, offsets, channels, channels), BF16),
            pltpu.VMEM((offsets, rows, width), BF16),
            pltpu.VMEM((peers * cap, rows), BF16),
            pltpu.VMEM((2, rows, channels), BF16),
            pltpu.VMEM((2, rows, channels), BF16),
            pltpu.VMEM((rows, channels), F32),
            pltpu.VMEM((peers, 1, lanes), jnp.int32),
            pltpu.VMEM((2, peers, cap, channels), BF16),
            pltpu.VMEM((2, peers, cap, channels), BF16),
            pltpu.SemaphoreType.DMA,
            pltpu.SemaphoreType.DMA,
            pltpu.SemaphoreType.DMA((2,)),
            pltpu.SemaphoreType.DMA((2,)),
            pltpu.SemaphoreType.DMA((2,)),
            pltpu.SemaphoreType.DMA((2,)),
            pltpu.SemaphoreType.DMA((5,)),
        ],
        compiler_params=pltpu.CompilerParams(
            collective_id=0, has_side_effects=True, vmem_limit_bytes=60 * 1024 * 1024
        ),
        name="autoencoder",
    )(features, weights, conv_bias, rulebook, border, wanted)


def solution(mesh):
    return jax.shard_map(
        body,
        mesh=mesh,
        in_specs=(
            P(None, "space", None),
            P("phase", None, None, None),
            P(),
            P("space", None),
            P("space", None),
            P("space", None, None),
        ),
        out_specs=P("phase", None, "space", None),
        check_vma=False,
    )
```
